32 devices in a mesh: dp: 2 (over x), ep: 4 (over z), tp: 4 (over y, core).
Axes of the slice: x: 2, y: 2, z: 4, core: 2. Of those that a mesh axis runs over, the one named last changes fastest.
Arguments:
- X: bfloat16 [16384, 1024], P(('dp', 'ep', 'tp')), parts along dimension 0
- idx: int32 [16384, 8], P(('dp', 'ep', 'tp')), parts along dimension 0
- g: float32 [16384, 8], P(('dp', 'ep', 'tp')), parts along dimension 0
- W1: bfloat16 [32, 1024, 512], P('ep', None, 'tp')
- W3: bfloat16 [32, 1024, 512], P('ep', None, 'tp')
- W2: bfloat16 [32, 512, 1024], P('ep', 'tp')
Outputs:
- output: bfloat16 [16384, 1024], P(('dp', 'ep', 'tp')), parts along dimension 0
There are 2 independent parts. The reference program is written for one: setup_inputs(seed, part) draws one part's arguments, and reference() takes and returns one part's arrays. A program takes and returns all parts, laid end to end along the dimension named above; an argument that names none is the same for every part.
All inputs are finite; a program needn't handle non-finite values.
Results may differ from the reference program's by a relative error of at most 0.0102037.
Values are sent between devices in bfloat16 or wider.
A program may use at most 1 GiB of HBM per device.

```python
import jax
import jax.numpy as jnp
from jax import lax

D = 1024
F = 512
E = 32
TOP = 8
T_LOC = 512
NDEV = 16
C = 2 * TOP * T_LOC // E
T = NDEV * T_LOC


def _weights(key, shape, fan):
    def one(k):
        return (jax.random.normal(k, shape, jnp.float32) * fan ** -0.5).astype(jnp.bfloat16)
    return lax.map(one, jax.random.split(key, E))


def setup_inputs(seed: int = 0, part: int = 0) -> dict:
    key = jax.random.PRNGKey(seed)
    kdata, kw = jax.random.split(key)
    kx, kr, kg = jax.random.split(jax.random.fold_in(kdata, part), 3)
    k1, k3, k2 = jax.random.split(kw, 3)
    x = jax.random.normal(kx, (T, D), jnp.float32).astype(jnp.bfloat16)
    expert_rank = jnp.arange(E, dtype=jnp.uint32)
    wait_scale = jnp.uint32(512) - (jnp.uint32(256) * expert_rank) // jnp.uint32(max(E - 1, 1))
    wait_time = (jax.random.bits(jax.random.fold_in(kr, 7), (T, E), jnp.uint32) >> 10) * wait_scale[None, :]
    idx = jnp.argsort(wait_time, axis=1)[:, :TOP].astype(jnp.int32)
    g = jax.random.uniform(kg, (T, TOP), jnp.float32, 0.25, 1.0)
    return {"X": x, "idx": idx, "g": g,
            "W1": _weights(k1, (D, F), D), "W3": _weights(k3, (D, F), D), "W2": _weights(k2, (F, D), F)}


def _slots(ids):
    oh = (ids[:, None] == jnp.arange(E, dtype=jnp.int32)[None, :]).astype(jnp.int32)
    return jnp.sum(oh * (jnp.cumsum(oh, axis=0) - 1), axis=1)


def reference(X, idx, g, W1, W3, W2):
    ids = idx.reshape(NDEV, T_LOC * TOP)
    s = jax.vmap(_slots)(ids)
    keep = s < C
    dest = jnp.where(keep, ids * C + s, E * C)
    xr = jnp.repeat(X.reshape(NDEV, T_LOC, D), TOP, axis=1)
    buf = jax.vmap(lambda x, dd: jnp.zeros((E * C, D), X.dtype).at[dd].set(x, mode="drop"))(xr, dest)
    buf = buf.reshape(NDEV, E, C, D).transpose(1, 0, 2, 3)

    def expert(a):
        xb, w1, w3, w2 = a

        def rows(x):
            h1 = jnp.dot(x, w1, preferred_element_type=jnp.float32)
            h3 = jnp.dot(x, w3, preferred_element_type=jnp.float32)
            h = (jax.nn.silu(h1) * h3).astype(jnp.bfloat16)
            return jnp.dot(h, w2, preferred_element_type=jnp.float32).astype(jnp.bfloat16)
        return lax.map(rows, xb)

    yb = lax.map(expert, (buf, W1, W3, W2))
    yb = yb.transpose(1, 0, 2, 3).reshape(NDEV, E * C, D)
    ysel = jax.vmap(lambda y, dd: y[jnp.minimum(dd, E * C - 1)])(yb, dest)
    wgt = jnp.where(keep, g.reshape(NDEV, T_LOC * TOP), 0.0)
    out = jnp.sum(ysel.astype(jnp.float32).reshape(NDEV, T_LOC, TOP, D) * wgt.reshape(NDEV, T_LOC, TOP, 1), axis=2)
    return out.reshape(T, D).astype(jnp.bfloat16)
```

```python
import jax
import jax.numpy as jnp
from jax import lax
from jax.sharding import PartitionSpec as P

CF = 2


def _dense_gates(idx, g, n_exp, cap):
    t_loc = idx.shape[0]
    hit = idx[:, :, None] == jnp.arange(n_exp, dtype=jnp.int32)[None, None, :]
    multi = jnp.any(hit, axis=1)
    before = lax.broadcasted_iota(jnp.int32, (t_loc, t_loc), 1) < lax.broadcasted_iota(jnp.int32, (t_loc, t_loc), 0)
    slot = jnp.dot(before.astype(jnp.bfloat16), multi.astype(jnp.bfloat16), preferred_element_type=jnp.float32)
    gate = jnp.sum(jnp.where(hit, g[:, :, None], 0.0), axis=1)
    return jnp.where(slot < cap, gate, 0.0)


def solution(mesh):
    ep, tp = mesh.shape["ep"], mesh.shape["tp"]
    rows = P(("dp", "ep", "tp"), None)

    def local(x, idx, g, w1, w3, w2):
        t_loc, d = x.shape
        top = idx.shape[1]
        el = w1.shape[0]
        n_exp = el * ep
        cap = CF * top * t_loc // n_exp
        gates = _dense_gates(idx, g, n_exp, cap)
        gl = lax.all_to_all(gates.reshape(t_loc, ep, el).transpose(1, 0, 2), "ep", 0, 0, tiled=True).reshape(ep * t_loc, el)
        xa = lax.all_gather(x, "ep", axis=0, tiled=True)
        w13 = lax.all_gather(jnp.concatenate([w1, w3], axis=2), "tp", axis=0)
        w2a = lax.all_gather(w2, "tp", axis=0)
        f = w1.shape[2]
        acc = jnp.zeros((ep * t_loc, d), jnp.float32)
        for e in range(el):
            parts = []
            for s in range(tp):
                ab = jnp.dot(xa, w13[s, e], preferred_element_type=jnp.float32)
                parts.append((jax.nn.silu(ab[:, :f]) * ab[:, f:]).astype(jnp.bfloat16))
            h = jnp.concatenate(parts, axis=1)
            y = jnp.dot(h, w2a[:, e].reshape(tp * f, d), preferred_element_type=jnp.float32)
            acc = acc + gl[:, e:e + 1] * lax.reduce_precision(y, 8, 7)
        return lax.psum_scatter(acc, "ep", scatter_dimension=0, tiled=True).astype(jnp.bfloat16)

    return jax.shard_map(local, mesh=mesh,
                         in_specs=(rows, rows, rows, P("ep", None, "tp"), P("ep", None, "tp"), P("ep", "tp", None)),
                         out_specs=rows, check_vma=False)
```

```python
import functools

import jax
import jax.numpy as jnp
from jax import lax
from jax.experimental import pallas as pl
from jax.experimental.pallas import tpu as pltpu
from jax.sharding import PartitionSpec as P

CF = 2
MESH = pl.DeviceIdType.MESH
NSUB = 4
F32, BF16 = jnp.float32, jnp.bfloat16


def _kernel(cap, x_ref, idx_ref, g_ref, w1_ref, w3_ref, w2_ref, out_ref,
            w13, w2, xall, gsend, gall, gcols, part, from_back, from_fwd,
            ld_x, ld_w, own_s, own_r, y_s, y_r, x_s, x_r, yp_s, yp_r, xp_s, xp_r,
            t_s, t_r, g_s, g_r, r_s, rb_r, rf_r):
    T, D = x_ref.shape
    FL = w1_ref.shape[2]
    TOP = idx_ref.shape[1]
    EL = w1_ref.shape[0]
    KH, TH, TS = D // 2, T // 2, T // NSUB

    xx = lax.axis_index("dp")
    z = lax.axis_index("ep")
    t = lax.axis_index("tp")
    yy, core = t // 2, t % 2
    mate = 2 * yy + 1 - core
    across = 2 * (1 - yy) + core
    to_mate, to_y, to_x = {"tp": mate}, {"tp": across}, {"dp": 1 - xx}
    low = z < 2
    m = jnp.where(low, z, 3 - z)
    fz = jnp.where(low, z + 1, z - 1)
    bz = jnp.where(low, z - 1, z + 1)

    def real(dm):
        return jnp.where(low, dm, 3 - dm)

    def dest(pos):
        return real((m + 1 + pos) % 4)

    def remote(src, dst, ss, rs, dev):
        return pltpu.make_async_remote_copy(src_ref=src, dst_ref=dst, send_sem=ss, recv_sem=rs,
                                            device_id=dev, device_id_type=MESH)

    def piece(e, s, p):
        if p < 2:
            return w13.at[e, s, pl.ds(p * KH, KH)]
        return w2.at[e, pl.ds(pl.multiple_of(s * FL, FL), FL)]

    def load_x():
        return pltpu.make_async_copy(x_ref, xall.at[z], ld_x)

    def load_w(e):
        return (pltpu.make_async_copy(w1_ref.at[e], w13.at[e, t, :, pl.ds(0, FL)], ld_w.at[e, 0]),
                pltpu.make_async_copy(w3_ref.at[e], w13.at[e, t, :, pl.ds(FL, FL)], ld_w.at[e, 1]),
                pltpu.make_async_copy(w2_ref.at[e], w2.at[e, pl.ds(pl.multiple_of(t * FL, FL), FL)], ld_w.at[e, 2]))

    load_x().start()
    for k in range(EL // 2):
        for e in (2 * k + xx, 2 * k + 1 - xx):
            for c in load_w(e):
                c.start()

    barrier = pltpu.get_barrier_semaphore()
    for dev in (to_mate, to_y, to_x, {"ep": (z + 1) % 4}, {"ep": (z + 2) % 4}, {"ep": (z + 3) % 4}):
        pl.semaphore_signal(barrier, inc=1, device_id=dev, device_id_type=MESH)
    pl.semaphore_wait(barrier, 6)

    def own_copy(e, p):
        return remote(piece(e, t, p), piece(e, t, p), own_s.at[e, p], own_r.at[e, p], to_mate)

    def y_copy(k, p):
        return remote(piece(2 * k + xx, t, p), piece(2 * k + xx, t, p), y_s.at[k, p], y_r.at[k, p], to_y)

    def x_copy(k, p):
        r = piece(2 * k + xx, across, p)
        return remote(r, r, x_s.at[k, p], x_r.at[k, p], to_x)

    def yp_copy(k, p):
        r = piece(2 * k + xx, across, p)
        return remote(r, r, yp_s.at[k, p], yp_r.at[k, p], to_mate)

    def xp_copy(k, p):
        r = piece(2 * k + 1 - xx, across, p)
        return remote(r, r, xp_s.at[k, p], xp_r.at[k, p], to_mate)

    def row_copy(src, half, side, hop):
        r = xall.at[src, pl.ds(half * TH, TH)]
        to = {"ep": z + 1 if side == 0 else z - 1}
        return remote(r, r, t_s.at[side, hop, half], t_r.at[src, half], to)

    def rows_wait(src, half):
        r = xall.at[src, pl.ds(half * TH, TH)]
        remote(r, r, t_s.at[0, 0, half], t_r.at[src, half], {"ep": z}).wait_recv()

    def send_own_rows(half):
        @pl.when(z < 3)
        def _():
            row_copy(z, half, 0, 0).start()

        @pl.when(z > 0)
        def _():
            row_copy(z, half, 1, 0).start()

    def first_rows(half):
        @pl.when(m == 0)
        def _():
            rows_wait(dest(0), half)

        @pl.when(m == 1)
        def _():
            rows_wait(z - 1, half)
            row_copy(z - 1, half, 0, 1).start()
            rows_wait(z + 1, half)
            row_copy(z + 1, half, 1, 1).start()

    def second_rows(half):
        rows_wait(dest(1), half)

        @pl.when(z == 1)
        def _():
            row_copy(z + 2, half, 1, 2).start()

        @pl.when(z == 2)
        def _():
            row_copy(z - 2, half, 0, 2).start()

    def third_rows(half):
        @pl.when(m == 0)
        def _():
            rows_wait(dest(2), half)

    load_x().wait()
    send_own_rows(0)
    for k in range(EL // 2):
        e = 2 * k + xx
        for c in load_w(e):
            c.wait()
        for p in range(3):
            y_copy(k, p).start()
        for p in range(3):
            own_copy(e, p).start()

    lane = lax.broadcasted_iota(jnp.int32, (T, 128), 1)
    gate = jnp.zeros((T, 128), F32)
    chosen = jnp.zeros((T, 128), F32)
    for j in range(TOP):
        hit = idx_ref[:, j:j + 1] == lane
        gate = jnp.where(hit, g_ref[:, j:j + 1], gate)
        chosen = jnp.where(hit, 1.0, chosen)
    before = (lax.broadcasted_iota(jnp.int32, (T, T), 1) < lax.broadcasted_iota(jnp.int32, (T, T), 0))
    slot = jnp.dot(before.astype(F32).astype(BF16), chosen.astype(BF16), preferred_element_type=F32)
    gate = jnp.where(slot < float(cap), gate, 0.0)
    gate_t = gate.T
    for r in range(4):
        gsend[r] = gate_t[r * EL:(r + 1) * EL, :]

    def gate_copy(step):
        r = (z + step) % 4
        return remote(gsend.at[r], gall.at[z], g_s.at[step - 1], g_r.at[step - 1], {"ep": r})

    for step in range(1, 4):
        gate_copy(step).start()
    send_own_rows(1)
    for k in range(EL // 2):
        e = 2 * k + 1 - xx
        for c in load_w(e):
            c.wait()
        for p in range(3):
            own_copy(e, p).start()
    part[...] = jnp.zeros_like(part)

    def gate_columns():
        gall[z] = gsend[z]
        for step in range(1, 4):
            gate_copy(step).wait_recv()
        for r in range(4):
            wide = jnp.concatenate([gall[r], jnp.zeros((128 - EL, T), F32)], axis=0)
            gcols[r] = wide.T

    def ready(j):
        k = j // 2
        e = 2 * k + (xx if j % 2 == 0 else 1 - xx)
        for p in range(3):
            own_copy(e, p).wait_recv()
            (yp_copy if j % 2 == 0 else xp_copy)(k, p).wait_recv()

    def unit(j, pos):
        odd = j % 2
        e = (j // 2) * 2 + odd + xx - 2 * odd * xx
        d = dest(pos)
        rows = xall[d]
        hs = []
        for s in range(4):
            ab = jnp.dot(rows, w13[e, s], preferred_element_type=F32)
            hs.append((jax.nn.silu(ab[:, :FL]) * ab[:, FL:]).astype(BF16))
        h = jnp.concatenate(hs, axis=1)
        col = jnp.sum(jnp.where(lane == e, gcols[d], 0.0), axis=1, keepdims=True)
        nb = min(256, D)
        for n in range(D // nb):
            cols = pl.ds(n * nb, nb)
            y = jnp.dot(h, w2[e, :, cols], preferred_element_type=F32).astype(BF16).astype(F32)
            part[d, :, cols] = part[d, :, cols] + col * y

    def units(pos, lo, hi):
        if hi == lo + 1:
            unit(jnp.int32(lo), pos)
            return

        def body(j, c):
            unit(j, pos)
            return c

        lax.fori_loop(lo, hi, body, 0)

    n_slots = 3 * (EL // 2)
    for i in range(n_slots + 1):
        if i < n_slots:
            k, p = divmod(i, 3)
            y_copy(k, p).wait_recv()
            x_copy(k, p).start()
            yp_copy(k, p).start()
        if i >= 1:
            k, p = divmod(i - 1, 3)
            x_copy(k, p).wait_recv()
            xp_copy(k, p).start()
        if i == 2:
            first_rows(0)
        if i == 4:
            first_rows(1)
            gate_columns()
            ready(0)
            ready(1)
            units(0, 0, 2)
        if i == 6:
            second_rows(0)
            ready(2)
            ready(3)
            units(0, 2, 4)
        if i == 8:
            second_rows(1)
            units(1, 0, 2)
        if i == 9:
            units(1, 2, 4)
        if i == 10:
            ready(4)
            ready(5)
            units(1, 4, 6)
        if i == 11:
            ready(6)
            units(1, 6, 7)
    ready(7)
    units(1, 7, 8)

    def chunk(dm, s):
        return part.at[real(dm), pl.ds(pl.multiple_of(s * TS, TS), TS)]

    def sub(ref, i, s):
        return ref.at[i, pl.ds(pl.multiple_of(s * TS, TS), TS)]

    def edge_copy(n, dm, s):
        return remote(chunk(dm, s), sub(from_back, dm - 1, s), r_s.at[n, s], rb_r.at[dm - 1, s], {"ep": fz})

    def inner_copy(n, dm, s):
        return remote(chunk(dm, s), sub(from_fwd, 3 - dm, s), r_s.at[n, s], rf_r.at[3 - dm, s], {"ep": fz})

    def outer_copy(s):
        return remote(chunk(0, s), sub(from_fwd, 0, s), r_s.at[2, s], rf_r.at[0, s], {"ep": bz})

    def back_wait(i, s):
        r = sub(from_back, i, s)
        remote(r, r, r_s.at[0, s], rb_r.at[i, s], {"ep": fz}).wait_recv()

    def fwd_wait(i, s):
        r = sub(from_fwd, i, s)
        remote(r, r, r_s.at[0, s], rf_r.at[i, s], {"ep": fz}).wait_recv()

    def add(dm, ref, i, s):
        here = pl.ds(pl.multiple_of(s * TS, TS), TS)
        d = real(dm)
        part[d, here] = part[d, here] + ref[i, here]

    def pass_on(n, dm, s):
        back_wait(dm - 1, s)
        add(dm, from_back, dm - 1, s)
        inner_copy(n, dm, s).start()

    def pass_out(s):
        fwd_wait(0, s)
        add(0, from_fwd, 0, s)
        outer_copy(s).start()

    def every(fn):
        def body(s, c):
            fn(s)
            return c

        lax.fori_loop(0, NSUB, body, 0)

    @pl.when(m == 0)
    def _():
        every(lambda s: edge_copy(0, 2, s).start())

    for half in range(2):
        third_rows(half)

    def late(g, c):
        @pl.when((m == 1) & (g >= 1))
        def _():
            pass_on(0, 2, g - 1)

        pos = jnp.where(g == 0, 0, jnp.where(g <= 2, 2, 3))
        first = jnp.where(g == 0, 4, 4 * ((g + 1) % 2))

        def body(j, cc):
            unit(first + j, pos)
            return cc

        lax.fori_loop(0, 4, body, 0)

        @pl.when((m == 0) & (g == 2))
        def _():
            every(lambda s: edge_copy(1, 3, s).start())
            every(lambda s: edge_copy(2, 1, s).start())

        return c

    lax.fori_loop(0, NSUB + 1, late, 0)

    @pl.when(m == 1)
    def _():
        pass_on(1, 3, 0)

        def body(s, c):
            pass_on(1, 3, s)
            pass_out(s - 1)
            return c

        lax.fori_loop(1, NSUB, body, 0)
        pass_out(NSUB - 1)

        def last(s):
            here = pl.ds(pl.multiple_of(s * TS, TS), TS)
            fwd_wait(1, s)
            back_wait(0, s)
            out_ref[here] = (part[z, here] + from_back[0, here] + from_fwd[1, here]).astype(out_ref.dtype)

        every(last)

    @pl.when(m == 0)
    def _():
        def last(s):
            here = pl.ds(pl.multiple_of(s * TS, TS), TS)
            fwd_wait(0, s)
            out_ref[here] = (part[z, here] + from_fwd[0, here]).astype(out_ref.dtype)

        every(last)

    for k in range(EL // 2):
        for p in range(3):
            y_copy(k, p).wait_send()
            x_copy(k, p).wait_send()
            yp_copy(k, p).wait_send()
            xp_copy(k, p).wait_send()
            own_copy(2 * k, p).wait_send()
            own_copy(2 * k + 1, p).wait_send()
    for step in range(1, 4):
        gate_copy(step).wait_send()
    for half in range(2):
        @pl.when(z < 3)
        def _():
            row_copy(z, half, 0, 0).wait_send()

        @pl.when(z > 0)
        def _():
            row_copy(z, half, 1, 0).wait_send()

        @pl.when(m == 1)
        def _():
            row_copy(z - 1, half, 0, 1).wait_send()
            row_copy(z + 1, half, 1, 1).wait_send()

        @pl.when(z == 1)
        def _():
            row_copy(z + 2, half, 1, 2).wait_send()

        @pl.when(z == 2)
        def _():
            row_copy(z - 2, half, 0, 2).wait_send()

    @pl.when(m == 0)
    def _():
        for n, dm in ((0, 2), (1, 3), (2, 1)):
            every(lambda s: edge_copy(n, dm, s).wait_send())

    @pl.when(m == 1)
    def _():
        for n, dm in ((0, 2), (1, 3)):
            every(lambda s: inner_copy(n, dm, s).wait_send())
        every(lambda s: outer_copy(s).wait_send())


def solution(mesh):
    ep, tp = mesh.shape["ep"], mesh.shape["tp"]
    rows = P(("dp", "ep", "tp"), None)

    def local(x, idx, g, w1, w3, w2):
        T, D = x.shape
        top = idx.shape[1]
        EL, _, FL = w1.shape
        cap = CF * top * T // (EL * ep)
        any_spec = pl.BlockSpec(memory_space=pl.ANY)
        vmem_spec = pl.BlockSpec(memory_space=pltpu.VMEM)
        dma = pltpu.SemaphoreType.DMA
        half_e = EL // 2
        return pl.pallas_call(
            functools.partial(_kernel, cap),
            name="moe",
            out_shape=jax.ShapeDtypeStruct((T, D), x.dtype),
            in_specs=[any_spec, vmem_spec, vmem_spec, any_spec, any_spec, any_spec],
            out_specs=vmem_spec,
            scratch_shapes=[
                pltpu.VMEM((EL, tp, D, 2 * FL), BF16),
                pltpu.VMEM((EL, tp * FL, D), BF16),
                pltpu.VMEM((ep, T, D), BF16),
                pltpu.VMEM((ep, EL, T), F32),
                pltpu.VMEM((ep, EL, T), F32),
                pltpu.VMEM((ep, T, 128), F32),
                pltpu.VMEM((ep, T, D), F32),
                pltpu.VMEM((3, T, D), F32),
                pltpu.VMEM((2, T, D), F32),
                dma, dma((EL, 3)),
                dma((EL, 3)), dma((EL, 3)),
                dma((half_e, 3)), dma((half_e, 3)),
                dma((half_e, 3)), dma((half_e, 3)),
                dma((half_e, 3)), dma((half_e, 3)),
                dma((half_e, 3)), dma((half_e, 3)),
                dma((2, 3, 2)), dma((4, 2)),
                dma((3,)), dma((3,)),
                dma((3, NSUB)), dma((3, NSUB)), dma((2, NSUB)),
            ],
            compiler_params=pltpu.CompilerParams(collective_id=0, has_side_effects=True,
                                                 vmem_limit_bytes=67_043_328),
        )(x, idx, g, w1, w3, w2)

    return jax.shard_map(local, mesh=mesh,
                         in_specs=(rows, rows, rows, P("ep", None, "tp"), P("ep", None, "tp"), P("ep", "tp", None)),
                         out_specs=rows, check_vma=False)
```

```python
import functools

import jax
import jax.numpy as jnp
from jax import lax
from jax.experimental import pallas as pl
from jax.experimental.pallas import tpu as pltpu
from jax.sharding import PartitionSpec as P

CF = 2
MESH = pl.DeviceIdType.MESH
NSUB = 8
F32, BF16 = jnp.float32, jnp.bfloat16


def _kernel(cap, x_ref, idx_ref, g_ref, w1_ref, w3_ref, w2_ref, out_ref,
            w13, w2, xall, gsend, gall, gcols, part, from_back, from_fwd, done,
            ld_x, ld_w, own_s, own_r, y_s, y_r, x_s, x_r, yp_s, yp_r, xp_s, xp_r,
            t_s, t_r, g_s, g_r, r_s, rb_r, rf_r, d_s, d_r):
    T, D = x_ref.shape
    FL = w1_ref.shape[2]
    TOP = idx_ref.shape[0]
    EL = w1_ref.shape[0]
    KH, TH, TS = D // 2, T // 2, T // NSUB

    xx = lax.axis_index("dp")
    z = lax.axis_index("ep")
    t = lax.axis_index("tp")
    yy, core = t // 2, t % 2
    mate = 2 * yy + 1 - core
    across = 2 * (1 - yy) + core
    to_mate, to_y, to_x = {"tp": mate}, {"tp": across}, {"dp": 1 - xx}
    low = z < 2
    m = jnp.where(low, z, 3 - z)
    fz = jnp.where(low, z + 1, z - 1)
    bz = jnp.where(low, z - 1, z + 1)

    def real(dm):
        return jnp.where(low, dm, 3 - dm)

    def dest(pos):
        return real((m + 1 + pos) % 4)

    def remote(src, dst, ss, rs, dev):
        return pltpu.make_async_remote_copy(src_ref=src, dst_ref=dst, send_sem=ss, recv_sem=rs,
                                            device_id=dev, device_id_type=MESH)

    def piece(e, s, p):
        if p < 2:
            return w13.at[e, s, pl.ds(p * KH, KH)]
        return w2.at[e, pl.ds(pl.multiple_of(s * FL, FL), FL)]

    def load_x():
        return pltpu.make_async_copy(x_ref, xall.at[z], ld_x)

    def load_w(e):
        return (pltpu.make_async_copy(w1_ref.at[e], w13.at[e, t, :, pl.ds(0, FL)], ld_w.at[e, 0]),
                pltpu.make_async_copy(w3_ref.at[e], w13.at[e, t, :, pl.ds(FL, FL)], ld_w.at[e, 1]),
                pltpu.make_async_copy(w2_ref.at[e], w2.at[e, pl.ds(pl.multiple_of(t * FL, FL), FL)], ld_w.at[e, 2]))

    load_x().start()
    for k in range(EL // 2):
        for e in (2 * k + xx, 2 * k + 1 - xx):
            for c in load_w(e):
                c.start()

    barrier = pltpu.get_barrier_semaphore()
    for dev in (to_mate, to_y, to_x, {"ep": (z + 1) % 4}, {"ep": (z + 2) % 4}, {"ep": (z + 3) % 4}):
        pl.semaphore_signal(barrier, inc=1, device_id=dev, device_id_type=MESH)
    pl.semaphore_wait(barrier, 6)

    def own_copy(e, p):
        return remote(piece(e, t, p), piece(e, t, p), own_s.at[e, p], own_r.at[e, p], to_mate)

    def y_copy(k, p):
        return remote(piece(2 * k + xx, t, p), piece(2 * k + xx, t, p), y_s.at[k, p], y_r.at[k, p], to_y)

    def x_copy(k, p):
        r = piece(2 * k + xx, across, p)
        return remote(r, r, x_s.at[k, p], x_r.at[k, p], to_x)

    def yp_copy(k, p):
        r = piece(2 * k + xx, across, p)
        return remote(r, r, yp_s.at[k, p], yp_r.at[k, p], to_mate)

    def xp_copy(k, p):
        r = piece(2 * k + 1 - xx, across, p)
        return remote(r, r, xp_s.at[k, p], xp_r.at[k, p], to_mate)

    def row_copy(src, half, side, hop):
        r = xall.at[src, pl.ds(half * TH, TH)]
        to = {"ep": z + 1 if side == 0 else z - 1}
        return remote(r, r, t_s.at[side, hop, half], t_r.at[src, half], to)

    def rows_wait(src, half):
        r = xall.at[src, pl.ds(half * TH, TH)]
        remote(r, r, t_s.at[0, 0, half], t_r.at[src, half], {"ep": z}).wait_recv()

    def send_own_rows(half):
        @pl.when(z < 3)
        def _():
            row_copy(z, half, 0, 0).start()

        @pl.when(z > 0)
        def _():
            row_copy(z, half, 1, 0).start()

    def first_rows(half):
        @pl.when(m == 0)
        def _():
            rows_wait(dest(0), half)

        @pl.when(m == 1)
        def _():
            rows_wait(z - 1, half)
            row_copy(z - 1, half, 0, 1).start()
            rows_wait(z + 1, half)
            row_copy(z + 1, half, 1, 1).start()

    def second_rows(half):
        rows_wait(dest(1), half)

        @pl.when(z == 1)
        def _():
            row_copy(z + 2, half, 1, 2).start()

        @pl.when(z == 2)
        def _():
            row_copy(z - 2, half, 0, 2).start()

    def third_rows(half):
        @pl.when(m == 0)
        def _():
            rows_wait(dest(2), half)

    load_x().wait()
    send_own_rows(0)
    for k in range(EL // 2):
        e = 2 * k + xx
        for c in load_w(e):
            c.wait()
        for p in range(3):
            y_copy(k, p).start()
        for p in range(3):
            own_copy(e, p).start()

    NE = gsend.shape[0] * EL
    expert = lax.broadcasted_iota(jnp.int32, (NE, T), 0)
    gate = jnp.zeros((NE, T), F32)
    chosen = jnp.zeros((NE, T), F32)
    for j in range(TOP):
        hit = idx_ref[j:j + 1, :] == expert
        gate = jnp.where(hit, g_ref[j:j + 1, :], gate)
        chosen = jnp.where(hit, 1.0, chosen)
    before = (lax.broadcasted_iota(jnp.int32, (T, T), 0) < lax.broadcasted_iota(jnp.int32, (T, T), 1))
    slot = jnp.dot(chosen.astype(BF16), before.astype(F32).astype(BF16), preferred_element_type=F32)
    gate = jnp.where(slot < float(cap), gate, 0.0)
    for r in range(4):
        gsend[r] = gate[r * EL:(r + 1) * EL, :]

    def gate_copy(step):
        r = (z + step) % 4
        return remote(gsend.at[r], gall.at[z], g_s.at[step - 1], g_r.at[step - 1], {"ep": r})

    for step in range(1, 4):
        gate_copy(step).start()
    send_own_rows(1)
    for k in range(EL // 2):
        e = 2 * k + 1 - xx
        for c in load_w(e):
            c.wait()
        for p in range(3):
            own_copy(e, p).start()
    part[...] = jnp.zeros_like(part)

    lane = lax.broadcasted_iota(jnp.int32, (T, 128), 1)

    def gate_columns():
        gall[z] = gsend[z]
        for step in range(1, 4):
            gate_copy(step).wait_recv()
        for r in range(4):
            wide = jnp.concatenate([gall[r], jnp.zeros((128 - EL, T), F32)], axis=0)
            gcols[r] = wide.T

    def ready(j):
        k = j // 2
        e = 2 * k + (xx if j % 2 == 0 else 1 - xx)
        for p in range(3):
            own_copy(e, p).wait_recv()
            (yp_copy if j % 2 == 0 else xp_copy)(k, p).wait_recv()

    def unit(j, dm):
        odd = j % 2
        e = (j // 2) * 2 + odd + xx - 2 * odd * xx
        d = real(dm)
        rows = xall[d]
        hs = []
        for s in range(4):
            ab = jnp.dot(rows, w13[e, s], preferred_element_type=F32)
            hs.append((jax.nn.silu(ab[:, :FL]) * ab[:, FL:]).astype(BF16))
        h = jnp.concatenate(hs, axis=1)
        col = jnp.sum(jnp.where(lane == e, gcols[d], 0.0), axis=1, keepdims=True)
        nb = min(256, D)
        for n in range(D // nb):
            cols = pl.ds(n * nb, nb)
            y = jnp.dot(h, w2[e, :, cols], preferred_element_type=F32).astype(BF16).astype(F32)
            part[d, :, cols] = part[d, :, cols] + col * y

    def units(dm, lo, hi):
        def body(j, c):
            unit(j, dm)
            return c

        lax.fori_loop(lo, hi, body, 0)

    n_slots = 3 * (EL // 2)
    for i in range(n_slots + 1):
        if i < n_slots:
            k, p = divmod(i, 3)
            y_copy(k, p).wait_recv()
            x_copy(k, p).start()
            yp_copy(k, p).start()
        if i >= 1:
            k, p = divmod(i - 1, 3)
            x_copy(k, p).wait_recv()
            xp_copy(k, p).start()
        if i == 2:
            first_rows(0)
        if i == 4:
            first_rows(1)
            gate_columns()
            ready(0)
            ready(1)
            units(1, 0, 2)
        if i == 5:
            units(0, 0, 2)
        if i == 6:
            second_rows(0)
            ready(2)
            ready(3)
            units(1, 2, 4)
        if i == 7:
            units(0, 2, 4)
        if i == 8:
            second_rows(1)
            units(2, 0, 2)
        if i == 9:
            units(2, 2, 4)
        if i == 10:
            ready(4)
            ready(5)
            units(2, 4, 6)
        if i == 11:
            ready(6)
            units(2, 6, 7)
    ready(7)
    units(2, 7, 8)

    def at(s):
        return pl.ds(pl.multiple_of(s * TS, TS), TS)

    def edge_copy(n, s):
        dm = 2 + n
        return remote(part.at[real(dm), at(s)], from_back.at[n, at(s)], r_s.at[n, s], rb_r.at[n, s], {"ep": fz})

    def fwd_copy(n, s):
        dm = 2 + n
        return remote(part.at[real(dm), at(s)], from_fwd.at[1 - n, at(s)], r_s.at[n, s], rf_r.at[1 - n, s], {"ep": fz})

    def bwd_copy(n, s):
        dm = 1 - n
        return remote(part.at[real(dm), at(s)], from_fwd.at[dm, at(s)], r_s.at[2 + n, s], rf_r.at[dm, s], {"ep": bz})

    def done_copy(s):
        return remote(done.at[at(s)], out_ref.at[at(s)], d_s.at[s], d_r.at[s], {"ep": fz})

    def fwd_wait(dm, s):
        r = from_fwd.at[dm, at(s)]
        remote(r, r, r_s.at[0, s], rf_r.at[dm, s], {"ep": fz}).wait_recv()

    def pass_fwd(i):
        n, s = i // NSUB, i % NSUB
        edge_copy(n, s).wait_recv()
        d = real(2 + n)
        part[d, at(s)] = part[d, at(s)] + from_back[n, at(s)]
        fwd_copy(n, s).start()

    def pass_bwd(i):
        n, s = i // NSUB, i % NSUB
        fwd_wait(1 - n, s)
        d = real(1 - n)
        part[d, at(s)] = part[d, at(s)] + from_fwd[1 - n, at(s)]
        bwd_copy(n, s).start()

    def both(i):
        pass_fwd(i)
        pass_bwd(i - 1)

    def loop(lo, hi, fn):
        def body(s, c):
            fn(s)
            return c

        lax.fori_loop(lo, hi, body, 0)

    def every(fn):
        loop(0, NSUB, fn)

    @pl.when(m == 0)
    def _():
        every(lambda s: edge_copy(0, s).start())

    for half in range(2):
        third_rows(half)

    def late(g, c):
        @pl.when((m == 1) & (g == 1))
        def _():
            pass_fwd(0)

        @pl.when((m == 1) & (g >= 2))
        def _():
            loop(2 * g - 3, 2 * g - 1, both)

        dm = jnp.where(g == 0, 1, jnp.where(g == 3, 0, 3))
        first = jnp.where(g == 1, 0, 4)
        loop(first, first + 4, lambda j: unit(j, dm))

        @pl.when((m == 0) & (g == 2))
        def _():
            every(lambda s: edge_copy(1, s).start())

        return c

    lax.fori_loop(0, 4, late, 0)

    @pl.when(m == 1)
    def _():
        loop(5, 2 * NSUB, both)
        pass_bwd(2 * NSUB - 1)
        every(lambda s: done_copy(s).wait_recv())

    @pl.when(m == 0)
    def _():
        def finish(s):
            fwd_wait(1, s)
            done[at(s)] = (part[real(1), at(s)] + from_fwd[1, at(s)]).astype(done.dtype)
            done_copy(s).start()

        every(finish)

        def last(s):
            fwd_wait(0, s)
            out_ref[at(s)] = (part[z, at(s)] + from_fwd[0, at(s)]).astype(out_ref.dtype)

        every(last)

    for k in range(EL // 2):
        for p in range(3):
            y_copy(k, p).wait_send()
            x_copy(k, p).wait_send()
            yp_copy(k, p).wait_send()
            xp_copy(k, p).wait_send()
            own_copy(2 * k, p).wait_send()
            own_copy(2 * k + 1, p).wait_send()
    for step in range(1, 4):
        gate_copy(step).wait_send()
    for half in range(2):
        @pl.when(z < 3)
        def _():
            row_copy(z, half, 0, 0).wait_send()

        @pl.when(z > 0)
        def _():
            row_copy(z, half, 1, 0).wait_send()

        @pl.when(m == 1)
        def _():
            row_copy(z - 1, half, 0, 1).wait_send()
            row_copy(z + 1, half, 1, 1).wait_send()

        @pl.when(z == 1)
        def _():
            row_copy(z + 2, half, 1, 2).wait_send()

        @pl.when(z == 2)
        def _():
            row_copy(z - 2, half, 0, 2).wait_send()

    @pl.when(m == 0)
    def _():
        for n in range(2):
            every(lambda s: edge_copy(n, s).wait_send())
        every(lambda s: done_copy(s).wait_send())

    @pl.when(m == 1)
    def _():
        for n in range(2):
            every(lambda s: fwd_copy(n, s).wait_send())
            every(lambda s: bwd_copy(n, s).wait_send())


def solution(mesh):
    ep, tp = mesh.shape["ep"], mesh.shape["tp"]
    rows = P(("dp", "ep", "tp"), None)

    def local(x, idx, g, w1, w3, w2):
        T, D = x.shape
        top = idx.shape[1]
        EL, _, FL = w1.shape
        cap = CF * top * T // (EL * ep)
        any_spec = pl.BlockSpec(memory_space=pl.ANY)
        vmem_spec = pl.BlockSpec(memory_space=pltpu.VMEM)
        dma = pltpu.SemaphoreType.DMA
        half_e = EL // 2
        return pl.pallas_call(
            functools.partial(_kernel, cap),
            name="moe",
            out_shape=jax.ShapeDtypeStruct((T, D), x.dtype),
            in_specs=[any_spec, vmem_spec, vmem_spec, any_spec, any_spec, any_spec],
            out_specs=vmem_spec,
            scratch_shapes=[
                pltpu.VMEM((EL, tp, D, 2 * FL), BF16),
                pltpu.VMEM((EL, tp * FL, D), BF16),
                pltpu.VMEM((ep, T, D), BF16),
                pltpu.VMEM((ep, EL, T), F32),
                pltpu.VMEM((ep, EL, T), F32),
                pltpu.VMEM((ep, T, 128), F32),
                pltpu.VMEM((ep, T, D), F32),
                pltpu.VMEM((2, T, D), F32),
                pltpu.VMEM((2, T, D), F32),
                pltpu.VMEM((T, D), BF16),
                dma, dma((EL, 3)),
                dma((EL, 3)), dma((EL, 3)),
                dma((half_e, 3)), dma((half_e, 3)),
                dma((half_e, 3)), dma((half_e, 3)),
                dma((half_e, 3)), dma((half_e, 3)),
                dma((half_e, 3)), dma((half_e, 3)),
                dma((2, 3, 2)), dma((4, 2)),
                dma((3,)), dma((3,)),
                dma((4, NSUB)), dma((2, NSUB)), dma((2, NSUB)),
                dma((NSUB,)), dma((NSUB,)),
            ],
            compiler_params=pltpu.CompilerParams(collective_id=0, has_side_effects=True,
                                                 vmem_limit_bytes=67_043_328),
        )(x, idx.T, g.T, w1, w3, w2)

    return jax.shard_map(local, mesh=mesh,
                         in_specs=(rows, rows, rows, P("ep", None, "tp"), P("ep", None, "tp"), P("ep", "tp", None)),
                         out_specs=rows, check_vma=False)
```

```python
import functools

import jax
import jax.numpy as jnp
from jax import lax
from jax.experimental import pallas as pl
from jax.experimental.pallas import tpu as pltpu
from jax.sharding import PartitionSpec as P

CF = 2
MESH = pl.DeviceIdType.MESH
NSUB = 8
F32, BF16 = jnp.float32, jnp.bfloat16


def _kernel(cap, x_ref, idx_ref, g_ref, w1_ref, w3_ref, w2_ref, out_ref,
            idx_v, g_v, w13, w2, xall, gsend, gall, gcols, part, from_back, from_fwd, done,
            ld_i, ld_x, ld_w, own_s, own_r, y_s, y_r, x_s, x_r, yp_s, yp_r, xp_s, xp_r,
            t_s, t_r, g_s, g_r, r_s, rb_r, rf_r, d_s, d_r):
    T, D = x_ref.shape
    FL = w1_ref.shape[2]
    TOP = idx_ref.shape[0]
    EL = w1_ref.shape[0]
    KH, TH, TS = D // 2, T // 2, T // NSUB

    xx = lax.axis_index("dp")
    z = lax.axis_index("ep")
    t = lax.axis_index("tp")
    yy, core = t // 2, t % 2
    mate = 2 * yy + 1 - core
    across = 2 * (1 - yy) + core
    to_mate, to_y, to_x = {"tp": mate}, {"tp": across}, {"dp": 1 - xx}
    low = z < 2
    m = jnp.where(low, z, 3 - z)
    fz = jnp.where(low, z + 1, z - 1)
    bz = jnp.where(low, z - 1, z + 1)

    def real(dm):
        return jnp.where(low, dm, 3 - dm)

    def dest(pos):
        return real((m + 1 + pos) % 4)

    def remote(src, dst, ss, rs, dev):
        return pltpu.make_async_remote_copy(src_ref=src, dst_ref=dst, send_sem=ss, recv_sem=rs,
                                            device_id=dev, device_id_type=MESH)

    def piece(e, s, p):
        if p < 2:
            return w13.at[e, s, pl.ds(p * KH, KH)]
        return w2.at[e, pl.ds(pl.multiple_of(s * FL, FL), FL)]

    def load_i():
        return (pltpu.make_async_copy(idx_ref, idx_v, ld_i.at[0]), pltpu.make_async_copy(g_ref, g_v, ld_i.at[1]))

    def load_x():
        return pltpu.make_async_copy(x_ref, xall.at[z], ld_x)

    def load_w(e):
        return (pltpu.make_async_copy(w1_ref.at[e], w13.at[e, t, :, pl.ds(0, FL)], ld_w.at[e, 0]),
                pltpu.make_async_copy(w3_ref.at[e], w13.at[e, t, :, pl.ds(FL, FL)], ld_w.at[e, 1]),
                pltpu.make_async_copy(w2_ref.at[e], w2.at[e, pl.ds(pl.multiple_of(t * FL, FL), FL)], ld_w.at[e, 2]))

    load_x().start()
    for e in (xx, 1 - xx):
        for c in load_w(e):
            c.start()
    for c in load_i():
        c.start()
    for k in range(1, EL // 2):
        for e in (2 * k + xx, 2 * k + 1 - xx):
            for c in load_w(e):
                c.start()

    barrier = pltpu.get_barrier_semaphore()
    for dev in (to_mate, to_y, to_x, {"ep": (z + 1) % 4}, {"ep": (z + 2) % 4}, {"ep": (z + 3) % 4}):
        pl.semaphore_signal(barrier, inc=1, device_id=dev, device_id_type=MESH)
    pl.semaphore_wait(barrier, 6)

    LAST = (EL // 2 - 1, 5)

    def small(e, s, q):
        if q < 4:
            return w13.at[e, s, pl.ds(q * (KH // 2), KH // 2)]
        return w2.at[e, pl.ds(pl.multiple_of(s * FL + (q - 4) * (FL // 2), FL // 2), FL // 2)]

    def own_copy(e, p):
        return remote(piece(e, t, p), piece(e, t, p), own_s.at[e, p], own_r.at[e, p], to_mate)

    def y_copy(k, q):
        r = small(2 * k + xx, t, q)
        return remote(r, r, y_s.at[k, q], y_r.at[k, q], to_y)

    def x_copy(k, q):
        if (k, q) == LAST:
            r = small(2 * k + 1 - xx, t, q)
            return remote(r, r, x_s.at[k, q], x_r.at[k, q], to_y)
        r = small(2 * k + xx, across, q)
        return remote(r, r, x_s.at[k, q], x_r.at[k, q], to_x)

    def yp_copy(k, p):
        r = piece(2 * k + xx, across, p)
        return remote(r, r, yp_s.at[k, p], yp_r.at[k, p], to_mate)

    def xp_copy(k, p):
        r = piece(2 * k + 1 - xx, across, p)
        return remote(r, r, xp_s.at[k, p], xp_r.at[k, p], to_mate)

    def row_copy(src, half, side, hop):
        r = xall.at[src, pl.ds(half * TH, TH)]
        to = {"ep": z + 1 if side == 0 else z - 1}
        return remote(r, r, t_s.at[side, hop, half], t_r.at[src, half], to)

    def rows_wait(src, half):
        r = xall.at[src, pl.ds(half * TH, TH)]
        remote(r, r, t_s.at[0, 0, half], t_r.at[src, half], {"ep": z}).wait_recv()

    def send_own_rows(half):
        @pl.when(z < 3)
        def _():
            row_copy(z, half, 0, 0).start()

        @pl.when(z > 0)
        def _():
            row_copy(z, half, 1, 0).start()

    def first_rows(half):
        @pl.when(m == 0)
        def _():
            rows_wait(dest(0), half)

        @pl.when(m == 1)
        def _():
            rows_wait(z - 1, half)
            row_copy(z - 1, half, 0, 1).start()
            rows_wait(z + 1, half)
            row_copy(z + 1, half, 1, 1).start()

    def second_rows(half):
        rows_wait(dest(1), half)

        @pl.when(z == 1)
        def _():
            row_copy(z + 2, half, 1, 2).start()

        @pl.when(z == 2)
        def _():
            row_copy(z - 2, half, 0, 2).start()

    def third_rows(half):
        @pl.when(m == 0)
        def _():
            rows_wait(dest(2), half)

    load_x().wait()
    send_own_rows(0)
    for k in range(EL // 2):
        e = 2 * k + xx
        for c in load_w(e):
            c.wait()
        for q in range(6):
            y_copy(k, q).start()
        for p in range(3):
            own_copy(e, p).start()

    for c in load_i():
        c.wait()
    NE = gsend.shape[0] * EL
    expert = lax.broadcasted_iota(jnp.int32, (NE, T), 0)
    gate = jnp.zeros((NE, T), F32)
    chosen = jnp.zeros((NE, T), F32)
    for j in range(TOP):
        hit = idx_v[j:j + 1, :] == expert
        gate = jnp.where(hit, g_v[j:j + 1, :], gate)
        chosen = jnp.where(hit, 1.0, chosen)
    before = (lax.broadcasted_iota(jnp.int32, (T, T), 0) < lax.broadcasted_iota(jnp.int32, (T, T), 1))
    slot = jnp.dot(chosen.astype(BF16), before.astype(F32).astype(BF16), preferred_element_type=F32)
    gate = jnp.where(slot < float(cap), gate, 0.0)
    for r in range(4):
        gsend[r] = gate[r * EL:(r + 1) * EL, :]

    def gate_copy(step):
        r = (z + step) % 4
        return remote(gsend.at[r], gall.at[z], g_s.at[step - 1], g_r.at[step - 1], {"ep": r})

    for step in range(1, 4):
        gate_copy(step).start()
    send_own_rows(1)
    for k in range(EL // 2):
        e = 2 * k + 1 - xx
        for c in load_w(e):
            c.wait()
        for p in range(3):
            own_copy(e, p).start()
    x_copy(*LAST).start()
    part[...] = jnp.zeros_like(part)

    lane = lax.broadcasted_iota(jnp.int32, (T, 128), 1)

    def gate_columns():
        gall[z] = gsend[z]
        for step in range(1, 4):
            gate_copy(step).wait_recv()
        for r in range(4):
            wide = jnp.concatenate([gall[r], jnp.zeros((128 - EL, T), F32)], axis=0)
            gcols[r] = wide.T

    def ready(j):
        k = j // 2
        e = 2 * k + (xx if j % 2 == 0 else 1 - xx)
        for p in range(3):
            own_copy(e, p).wait_recv()
            (yp_copy if j % 2 == 0 else xp_copy)(k, p).wait_recv()

    def unit(j, dm):
        odd = j % 2
        e = (j // 2) * 2 + odd + xx - 2 * odd * xx
        d = real(dm)
        rows = xall[d]
        hs = []
        for s in range(4):
            ab = jnp.dot(rows, w13[e, s], preferred_element_type=F32)
            hs.append((jax.nn.silu(ab[:, :FL]) * ab[:, FL:]).astype(BF16))
        h = jnp.concatenate(hs, axis=1)
        col = jnp.sum(jnp.where(lane == e, gcols[d], 0.0), axis=1, keepdims=True)
        nb = min(256, D)
        for n in range(D // nb):
            cols = pl.ds(n * nb, nb)
            y = jnp.dot(h, w2[e, :, cols], preferred_element_type=F32).astype(BF16).astype(F32)
            part[d, :, cols] = part[d, :, cols] + col * y

    plan = {9: (1, 0), 10: (1, 1), 11: (0, 0), 12: (0, 1), 13: (1, 2), 14: (1, 3), 15: (0, 2), 16: (0, 3),
            17: (2, 0), 18: (2, 1), 19: (2, 2), 20: (2, 3), 21: (2, 4), 22: (2, 5), 24: (2, 6)}
    first_use = {9: 0, 10: 1, 13: 2, 14: 3, 21: 4, 22: 5, 24: 6}
    n_slots = 6 * (EL // 2)
    for i in range(n_slots + 1):
        if i < n_slots:
            k, q = divmod(i, 6)
            y_copy(k, q).wait_recv()
            if (k, q) != LAST:
                x_copy(k, q).start()
            if q % 2 == 1:
                yp_copy(k, q // 2).start()
        if i >= 1:
            k, q = divmod(i - 1, 6)
            if (k, q) != LAST:
                x_copy(k, q).wait_recv()
                if q % 2 == 1:
                    xp_copy(k, q // 2).start()
        if i == 5:
            first_rows(0)
        if i == 8:
            first_rows(1)
            gate_columns()
        if i == 13:
            second_rows(0)
        if i == 17:
            second_rows(1)
        if i in first_use:
            ready(first_use[i])
        if i in plan:
            unit(jnp.int32(plan[i][1]), plan[i][0])
    x_copy(*LAST).wait_recv()
    xp_copy(LAST[0], 2).start()
    ready(7)
    unit(jnp.int32(7), 2)

    def at(s):
        return pl.ds(pl.multiple_of(s * TS, TS), TS)

    def edge_copy(n, s):
        dm = 2 + n
        return remote(part.at[real(dm), at(s)], from_back.at[n, at(s)], r_s.at[n, s], rb_r.at[n, s], {"ep": fz})

    def fwd_copy(n, s):
        dm = 2 + n
        return remote(part.at[real(dm), at(s)], from_fwd.at[1 - n, at(s)], r_s.at[n, s], rf_r.at[1 - n, s], {"ep": fz})

    def bwd_copy(n, s):
        dm = 1 - n
        return remote(part.at[real(dm), at(s)], from_fwd.at[dm, at(s)], r_s.at[2 + n, s], rf_r.at[dm, s], {"ep": bz})

    def done_copy(s):
        return remote(done.at[at(s)], out_ref.at[at(s)], d_s.at[s], d_r.at[s], {"ep": fz})

    def fwd_wait(dm, s):
        r = from_fwd.at[dm, at(s)]
        remote(r, r, r_s.at[0, s], rf_r.at[dm, s], {"ep": fz}).wait_recv()

    def pass_fwd(i):
        n, s = i // NSUB, i % NSUB
        edge_copy(n, s).wait_recv()
        d = real(2 + n)
        part[d, at(s)] = part[d, at(s)] + from_back[n, at(s)]
        fwd_copy(n, s).start()

    def pass_bwd(i):
        n, s = i // NSUB, i % NSUB
        fwd_wait(1 - n, s)
        d = real(1 - n)
        part[d, at(s)] = part[d, at(s)] + from_fwd[1 - n, at(s)]
        bwd_copy(n, s).start()

    def both(i):
        pass_fwd(i)
        pass_bwd(i - 1)

    def loop(lo, hi, fn):
        def body(s, c):
            fn(s)
            return c

        lax.fori_loop(lo, hi, body, 0)

    def every(fn):
        loop(0, NSUB, fn)

    @pl.when(m == 0)
    def _():
        every(lambda s: edge_copy(0, s).start())

    for half in range(2):
        third_rows(half)

    def late(g, c):
        @pl.when((m == 1) & (g == 1))
        def _():
            pass_fwd(0)

        @pl.when((m == 1) & (g >= 2))
        def _():
            loop(2 * g - 3, 2 * g - 1, both)

        dm = jnp.where(g == 0, 1, jnp.where(g == 3, 0, 3))
        first = jnp.where(g == 1, 0, 4)
        loop(first, first + 4, lambda j: unit(j, dm))

        @pl.when((m == 0) & (g == 2))
        def _():
            every(lambda s: edge_copy(1, s).start())

        return c

    lax.fori_loop(0, 4, late, 0)

    @pl.when(m == 1)
    def _():
        loop(5, 2 * NSUB, both)
        pass_bwd(2 * NSUB - 1)
        every(lambda s: done_copy(s).wait_recv())

    @pl.when(m == 0)
    def _():
        def finish(s):
            fwd_wait(1, s)
            done[at(s)] = (part[real(1), at(s)] + from_fwd[1, at(s)]).astype(done.dtype)
            done_copy(s).start()

        every(finish)

        def last(s):
            fwd_wait(0, s)
            out_ref[at(s)] = (part[z, at(s)] + from_fwd[0, at(s)]).astype(out_ref.dtype)

        every(last)

    for k in range(EL // 2):
        for q in range(6):
            y_copy(k, q).wait_send()
            x_copy(k, q).wait_send()
        for p in range(3):
            yp_copy(k, p).wait_send()
            xp_copy(k, p).wait_send()
            own_copy(2 * k, p).wait_send()
            own_copy(2 * k + 1, p).wait_send()
    for step in range(1, 4):
        gate_copy(step).wait_send()
    for half in range(2):
        @pl.when(z < 3)
        def _():
            row_copy(z, half, 0, 0).wait_send()

        @pl.when(z > 0)
        def _():
            row_copy(z, half, 1, 0).wait_send()

        @pl.when(m == 1)
        def _():
            row_copy(z - 1, half, 0, 1).wait_send()
            row_copy(z + 1, half, 1, 1).wait_send()

        @pl.when(z == 1)
        def _():
            row_copy(z + 2, half, 1, 2).wait_send()

        @pl.when(z == 2)
        def _():
            row_copy(z - 2, half, 0, 2).wait_send()

    @pl.when(m == 0)
    def _():
        for n in range(2):
            every(lambda s: edge_copy(n, s).wait_send())
        every(lambda s: done_copy(s).wait_send())

    @pl.when(m == 1)
    def _():
        for n in range(2):
            every(lambda s: fwd_copy(n, s).wait_send())
            every(lambda s: bwd_copy(n, s).wait_send())


def solution(mesh):
    ep, tp = mesh.shape["ep"], mesh.shape["tp"]
    rows = P(("dp", "ep", "tp"), None)

    def local(x, idx, g, w1, w3, w2):
        T, D = x.shape
        top = idx.shape[1]
        EL, _, FL = w1.shape
        cap = CF * top * T // (EL * ep)
        hbm_spec = pl.BlockSpec(memory_space=pltpu.MemorySpace.HBM)
        vmem_spec = pl.BlockSpec(memory_space=pltpu.VMEM)
        dma = pltpu.SemaphoreType.DMA
        half_e = EL // 2
        return pl.pallas_call(
            functools.partial(_kernel, cap),
            name="moe",
            out_shape=jax.ShapeDtypeStruct((T, D), x.dtype),
            in_specs=[hbm_spec] * 6,
            out_specs=vmem_spec,
            scratch_shapes=[
                pltpu.VMEM((top, T), jnp.int32),
                pltpu.VMEM((top, T), F32),
                pltpu.VMEM((EL, tp, D, 2 * FL), BF16),
                pltpu.VMEM((EL, tp * FL, D), BF16),
                pltpu.VMEM((ep, T, D), BF16),
                pltpu.VMEM((ep, EL, T), F32),
                pltpu.VMEM((ep, EL, T), F32),
                pltpu.VMEM((ep, T, 128), F32),
                pltpu.VMEM((ep, T, D), F32),
                pltpu.VMEM((2, T, D), F32),
                pltpu.VMEM((2, T, D), F32),
                pltpu.VMEM((T, D), BF16),
                dma((2,)), dma, dma((EL, 3)),
                dma((EL, 3)), dma((EL, 3)),
                dma((half_e, 6)), dma((half_e, 6)),
                dma((half_e, 6)), dma((half_e, 6)),
                dma((half_e, 3)), dma((half_e, 3)),
                dma((half_e, 3)), dma((half_e, 3)),
                dma((2, 3, 2)), dma((4, 2)),
                dma((3,)), dma((3,)),
                dma((4, NSUB)), dma((2, NSUB)), dma((2, NSUB)),
                dma((NSUB,)), dma((NSUB,)),
            ],
            compiler_params=pltpu.CompilerParams(collective_id=0, has_side_effects=True,
                                                 vmem_limit_bytes=52 << 20),
        )(x, idx.T, g.T, w1, w3, w2)

    return jax.shard_map(local, mesh=mesh,
                         in_specs=(rows, rows, rows, P("ep", None, "tp"), P("ep", None, "tp"), P("ep", "tp", None)),
                         out_specs=rows, check_vma=False)
```

```python
import functools

import jax
import jax.numpy as jnp
from jax import lax
from jax.experimental import pallas as pl
from jax.experimental.pallas import tpu as pltpu
from jax.sharding import PartitionSpec as P

CF = 2
MESH = pl.DeviceIdType.MESH
NSUB = 8
F32, BF16 = jnp.float32, jnp.bfloat16


def _kernel(cap, x_ref, idx_ref, g_ref, w1_ref, w3_ref, w2_ref, out_ref,
            w13, w2, xall, gsend, gall, gcols, part, from_back, from_fwd, done,
            ld_x, ld_w, own_s, own_r, y_s, y_r, x_s, x_r, yp_s, yp_r, xp_s, xp_r,
            t_s, t_r, g_s, g_r, r_s, rb_r, rf_r, d_s, d_r):
    T, D = x_ref.shape
    FL = w1_ref.shape[2]
    TOP = idx_ref.shape[0]
    EL = w1_ref.shape[0]
    KH, TH, TS = D // 2, T // 2, T // NSUB

    xx = lax.axis_index("dp")
    z = lax.axis_index("ep")
    t = lax.axis_index("tp")
    yy, core = t // 2, t % 2
    mate = 2 * yy + 1 - core
    across = 2 * (1 - yy) + core
    to_mate, to_y, to_x = {"tp": mate}, {"tp": across}, {"dp": 1 - xx}
    low = z < 2
    m = jnp.where(low, z, 3 - z)
    fz = jnp.where(low, z + 1, z - 1)
    bz = jnp.where(low, z - 1, z + 1)

    def real(dm):
        return jnp.where(low, dm, 3 - dm)

    def dest(pos):
        return real((m + 1 + pos) % 4)

    def remote(src, dst, ss, rs, dev):
        return pltpu.make_async_remote_copy(src_ref=src, dst_ref=dst, send_sem=ss, recv_sem=rs,
                                            device_id=dev, device_id_type=MESH)

    def piece(e, s, p):
        if p < 2:
            return w13.at[e, s, pl.ds(p * KH, KH)]
        return w2.at[e, pl.ds(pl.multiple_of(s * FL, FL), FL)]

    def load_x():
        return pltpu.make_async_copy(x_ref, xall.at[z], ld_x)

    def load_w(e):
        return (pltpu.make_async_copy(w1_ref.at[e], w13.at[e, t, :, pl.ds(0, FL)], ld_w.at[e, 0]),
                pltpu.make_async_copy(w3_ref.at[e], w13.at[e, t, :, pl.ds(FL, FL)], ld_w.at[e, 1]),
                pltpu.make_async_copy(w2_ref.at[e], w2.at[e, pl.ds(pl.multiple_of(t * FL, FL), FL)], ld_w.at[e, 2]))

    load_x().start()
    for k in range(EL // 2):
        for e in (2 * k + xx, 2 * k + 1 - xx):
            for c in load_w(e):
                c.start()

    barrier = pltpu.get_barrier_semaphore()
    for dev in (to_mate, to_y, to_x, {"ep": (z + 1) % 4}, {"ep": (z + 2) % 4}, {"ep": (z + 3) % 4}):
        pl.semaphore_signal(barrier, inc=1, device_id=dev, device_id_type=MESH)
    pl.semaphore_wait(barrier, 6)

    def own_copy(e, p):
        return remote(piece(e, t, p), piece(e, t, p), own_s.at[e, p], own_r.at[e, p], to_mate)

    def y_copy(k, p):
        return remote(piece(2 * k + xx, t, p), piece(2 * k + xx, t, p), y_s.at[k, p], y_r.at[k, p], to_y)

    def x_copy(k, p):
        r = piece(2 * k + xx, across, p)
        return remote(r, r, x_s.at[k, p], x_r.at[k, p], to_x)

    def yp_copy(k, p):
        r = piece(2 * k + xx, across, p)
        return remote(r, r, yp_s.at[k, p], yp_r.at[k, p], to_mate)

    def xp_copy(k, p):
        r = piece(2 * k + 1 - xx, across, p)
        return remote(r, r, xp_s.at[k, p], xp_r.at[k, p], to_mate)

    def row_copy(src, half, side, hop):
        r = xall.at[src, pl.ds(half * TH, TH)]
        to = {"ep": z + 1 if side == 0 else z - 1}
        return remote(r, r, t_s.at[side, hop, half], t_r.at[src, half], to)

    def rows_wait(src, half):
        r = xall.at[src, pl.ds(half * TH, TH)]
        remote(r, r, t_s.at[0, 0, half], t_r.at[src, half], {"ep": z}).wait_recv()

    def send_own_rows(half):
        @pl.when(z < 3)
        def _():
            row_copy(z, half, 0, 0).start()

        @pl.when(z > 0)
        def _():
            row_copy(z, half, 1, 0).start()

    def first_rows(half):
        @pl.when(m == 0)
        def _():
            rows_wait(dest(0), half)

        @pl.when(m == 1)
        def _():
            rows_wait(z - 1, half)
            row_copy(z - 1, half, 0, 1).start()
            rows_wait(z + 1, half)
            row_copy(z + 1, half, 1, 1).start()

    def second_rows(half):
        rows_wait(dest(1), half)

        @pl.when(z == 1)
        def _():
            row_copy(z + 2, half, 1, 2).start()

        @pl.when(z == 2)
        def _():
            row_copy(z - 2, half, 0, 2).start()

    def third_rows(half):
        @pl.when(m == 0)
        def _():
            rows_wait(dest(2), half)

    load_x().wait()
    send_own_rows(0)
    for k in range(EL // 2):
        e = 2 * k + xx
        for c in load_w(e):
            c.wait()
        for p in range(3):
            y_copy(k, p).start()
        for p in range(3):
            own_copy(e, p).start()

    NE = gsend.shape[0] * EL
    expert = lax.broadcasted_iota(jnp.int32, (NE, T), 0)
    gate = jnp.zeros((NE, T), F32)
    chosen = jnp.zeros((NE, T), F32)
    for j in range(TOP):
        hit = idx_ref[j:j + 1, :] == expert
        gate = jnp.where(hit, g_ref[j:j + 1, :], gate)
        chosen = jnp.where(hit, 1.0, chosen)
    before = (lax.broadcasted_iota(jnp.int32, (T, T), 0) < lax.broadcasted_iota(jnp.int32, (T, T), 1))
    slot = jnp.dot(chosen.astype(BF16), before.astype(F32).astype(BF16), preferred_element_type=F32)
    gate = jnp.where(slot < float(cap), gate, 0.0)
    for r in range(4):
        gsend[r] = gate[r * EL:(r + 1) * EL, :]

    def gate_copy(step):
        r = (z + step) % 4
        return remote(gsend.at[r], gall.at[z], g_s.at[step - 1], g_r.at[step - 1], {"ep": r})

    for step in range(1, 4):
        gate_copy(step).start()
    send_own_rows(1)
    for k in range(EL // 2):
        e = 2 * k + 1 - xx
        for c in load_w(e):
            c.wait()
        for p in range(3):
            own_copy(e, p).start()
    part[...] = jnp.zeros_like(part)

    lane = lax.broadcasted_iota(jnp.int32, (T, 128), 1)

    def gate_columns():
        gall[z] = gsend[z]
        for step in range(1, 4):
            gate_copy(step).wait_recv()
        for r in range(4):
            wide = jnp.concatenate([gall[r], jnp.zeros((128 - EL, T), F32)], axis=0)
            gcols[r] = wide.T

    def ready(j):
        k = j // 2
        e = 2 * k + (xx if j % 2 == 0 else 1 - xx)
        for p in range(3):
            own_copy(e, p).wait_recv()
            (yp_copy if j % 2 == 0 else xp_copy)(k, p).wait_recv()

    def unit(j, dm):
        odd = j % 2
        e = (j // 2) * 2 + odd + xx - 2 * odd * xx
        d = real(dm)
        rows = xall[d]
        hs = []
        for s in range(4):
            ab = jnp.dot(rows, w13[e, s], preferred_element_type=F32)
            hs.append((jax.nn.silu(ab[:, :FL]) * ab[:, FL:]).astype(BF16))
        h = jnp.concatenate(hs, axis=1)
        col = jnp.sum(jnp.where(lane == e, gcols[d], 0.0), axis=1, keepdims=True)
        nb = min(256, D)
        for n in range(D // nb):
            cols = pl.ds(n * nb, nb)
            y = jnp.dot(h, w2[e, :, cols], preferred_element_type=F32).astype(BF16).astype(F32)
            part[d, :, cols] = part[d, :, cols] + col * y

    def units(dm, lo, hi):
        def body(j, c):
            unit(j, dm)
            return c

        lax.fori_loop(lo, hi, body, 0)

    n_slots = 3 * (EL // 2)
    for i in range(n_slots + 1):
        if i < n_slots:
            k, p = divmod(i, 3)
            y_copy(k, p).wait_recv()
            x_copy(k, p).start()
            yp_copy(k, p).start()
        if i >= 1:
            k, p = divmod(i - 1, 3)
            x_copy(k, p).wait_recv()
            xp_copy(k, p).start()
        if i == 2:
            first_rows(0)
        if i == 4:
            first_rows(1)
            gate_columns()
            ready(0)
            ready(1)
            units(1, 0, 2)
        if i == 6:
            second_rows(0)
            ready(2)
            ready(3)
            units(1, 2, 4)
        if i == 8:
            second_rows(1)
            units(2, 0, 2)
        if i == 9:
            units(2, 2, 4)
        if i == 10:
            ready(4)
            ready(5)
            units(2, 4, 6)
        if i == 11:
            ready(6)
            units(2, 6, 7)
    ready(7)
    units(2, 7, 8)

    def at(s):
        return pl.ds(pl.multiple_of(s * TS, TS), TS)

    def edge_copy(n, s):
        dm = 2 + n
        return remote(part.at[real(dm), at(s)], from_back.at[n, at(s)], r_s.at[n, s], rb_r.at[n, s], {"ep": fz})

    def fwd_copy(n, s):
        dm = 2 + n
        return remote(part.at[real(dm), at(s)], from_fwd.at[1 - n, at(s)], r_s.at[n, s], rf_r.at[1 - n, s], {"ep": fz})

    def bwd_copy(n, s):
        dm = 1 - n
        return remote(part.at[real(dm), at(s)], from_fwd.at[dm, at(s)], r_s.at[2 + n, s], rf_r.at[dm, s], {"ep": bz})

    def done_copy(s):
        return remote(done.at[at(s)], out_ref.at[at(s)], d_s.at[s], d_r.at[s], {"ep": fz})

    def fwd_wait(dm, s):
        r = from_fwd.at[dm, at(s)]
        remote(r, r, r_s.at[0, s], rf_r.at[dm, s], {"ep": fz}).wait_recv()

    def pass_fwd(i):
        n, s = i // NSUB, i % NSUB
        edge_copy(n, s).wait_recv()
        d = real(2 + n)
        part[d, at(s)] = part[d, at(s)] + from_back[n, at(s)]
        fwd_copy(n, s).start()

    def pass_bwd(i):
        n, s = i // NSUB, i % NSUB
        fwd_wait(1 - n, s)
        d = real(1 - n)
        part[d, at(s)] = part[d, at(s)] + from_fwd[1 - n, at(s)]
        bwd_copy(n, s).start()

    def both(i):
        pass_fwd(i)
        pass_bwd(i - 1)

    def loop(lo, hi, fn):
        def body(s, c):
            fn(s)
            return c

        lax.fori_loop(lo, hi, body, 0)

    def every(fn):
        loop(0, NSUB, fn)

    @pl.when(m == 0)
    def _():
        every(lambda s: edge_copy(0, s).start())

    for half in range(2):
        third_rows(half)

    def late(g, c):
        @pl.when((m == 1) & (g == 1))
        def _():
            pass_fwd(0)

        @pl.when((m == 1) & (g >= 2))
        def _():
            loop(2 * g - 3, 2 * g - 1, both)

        dm = jnp.where(g == 0, 1, jnp.where(g == 3, 0, 3))
        first = jnp.where((g == 1) | (g == 3), 0, 4)
        loop(first, jnp.where(g == 1, 4, 8), lambda j: unit(j, dm))

        @pl.when((m == 0) & (g == 2))
        def _():
            every(lambda s: edge_copy(1, s).start())

        return c

    lax.fori_loop(0, 4, late, 0)

    @pl.when(m == 1)
    def _():
        loop(5, 2 * NSUB, both)
        pass_bwd(2 * NSUB - 1)
        every(lambda s: done_copy(s).wait_recv())

    @pl.when(m == 0)
    def _():
        def finish(s):
            fwd_wait(1, s)
            done[at(s)] = (part[real(1), at(s)] + from_fwd[1, at(s)]).astype(done.dtype)
            done_copy(s).start()

        every(finish)

        def last(s):
            fwd_wait(0, s)
            out_ref[at(s)] = (part[z, at(s)] + from_fwd[0, at(s)]).astype(out_ref.dtype)

        every(last)

    for k in range(EL // 2):
        for p in range(3):
            y_copy(k, p).wait_send()
            x_copy(k, p).wait_send()
            yp_copy(k, p).wait_send()
            xp_copy(k, p).wait_send()
            own_copy(2 * k, p).wait_send()
            own_copy(2 * k + 1, p).wait_send()
    for step in range(1, 4):
        gate_copy(step).wait_send()
    for half in range(2):
        @pl.when(z < 3)
        def _():
            row_copy(z, half, 0, 0).wait_send()

        @pl.when(z > 0)
        def _():
            row_copy(z, half, 1, 0).wait_send()

        @pl.when(m == 1)
        def _():
            row_copy(z - 1, half, 0, 1).wait_send()
            row_copy(z + 1, half, 1, 1).wait_send()

        @pl.when(z == 1)
        def _():
            row_copy(z + 2, half, 1, 2).wait_send()

        @pl.when(z == 2)
        def _():
            row_copy(z - 2, half, 0, 2).wait_send()

    @pl.when(m == 0)
    def _():
        for n in range(2):
            every(lambda s: edge_copy(n, s).wait_send())
        every(lambda s: done_copy(s).wait_send())

    @pl.when(m == 1)
    def _():
        for n in range(2):
            every(lambda s: fwd_copy(n, s).wait_send())
            every(lambda s: bwd_copy(n, s).wait_send())


def solution(mesh):
    ep, tp = mesh.shape["ep"], mesh.shape["tp"]
    rows = P(("dp", "ep", "tp"), None)

    def local(x, idx, g, w1, w3, w2):
        T, D = x.shape
        top = idx.shape[1]
        EL, _, FL = w1.shape
        cap = CF * top * T // (EL * ep)
        any_spec = pl.BlockSpec(memory_space=pl.ANY)
        vmem_spec = pl.BlockSpec(memory_space=pltpu.VMEM)
        dma = pltpu.SemaphoreType.DMA
        half_e = EL // 2
        return pl.pallas_call(
            functools.partial(_kernel, cap),
            name="moe",
            out_shape=jax.ShapeDtypeStruct((T, D), x.dtype),
            in_specs=[any_spec, vmem_spec, vmem_spec, any_spec, any_spec, any_spec],
            out_specs=vmem_spec,
            scratch_shapes=[
                pltpu.VMEM((EL, tp, D, 2 * FL), BF16),
                pltpu.VMEM((EL, tp * FL, D), BF16),
                pltpu.VMEM((ep, T, D), BF16),
                pltpu.VMEM((ep, EL, T), F32),
                pltpu.VMEM((ep, EL, T), F32),
                pltpu.VMEM((ep, T, 128), F32),
                pltpu.VMEM((ep, T, D), F32),
                pltpu.VMEM((2, T, D), F32),
                pltpu.VMEM((2, T, D), F32),
                pltpu.VMEM((T, D), BF16),
                dma, dma((EL, 3)),
                dma((EL, 3)), dma((EL, 3)),
                dma((half_e, 3)), dma((half_e, 3)),
                dma((half_e, 3)), dma((half_e, 3)),
                dma((half_e, 3)), dma((half_e, 3)),
                dma((half_e, 3)), dma((half_e, 3)),
                dma((2, 3, 2)), dma((4, 2)),
                dma((3,)), dma((3,)),
                dma((4, NSUB)), dma((2, NSUB)), dma((2, NSUB)),
                dma((NSUB,)), dma((NSUB,)),
            ],
            compiler_params=pltpu.CompilerParams(collective_id=0, has_side_effects=True,
                                                 vmem_limit_bytes=52 << 20),
        )(x, idx.T, g.T, w1, w3, w2)

    return jax.shard_map(local, mesh=mesh,
                         in_specs=(rows, rows, rows, P("ep", None, "tp"), P("ep", None, "tp"), P("ep", "tp", None)),
                         out_specs=rows, check_vma=False)
```
